32 devices in a mesh: seq: 16 (over z, y, core), fsdp: 2 (over x).
Axes of the slice: x: 2, y: 2, z: 4, core: 2. Of those that a mesh axis runs over, the one named last changes fastest.
Arguments:
- residual: bfloat16 [2, 1024, 1440], P('fsdp', 'seq'), may hold values from -40 to 40
- queries: bfloat16 [2, 1024, 2048], P('fsdp', 'seq'), may hold values from -64 to 64
- key_rows: bfloat16 [2, 1024, 256], P('fsdp', 'seq'), may hold values from -16 to 16
- values: bfloat16 [2, 1024, 256], P('fsdp', 'seq'), may hold values from -1 to 2
- attention_sinks: float32 [32], replicated, may hold values from 0 to 6
- out_weight: bfloat16 [2048, 1440], P('seq', 'fsdp'), may hold values from -0.125 to 0.125
- norm_gain: bfloat16 [1440], replicated, may hold values from 0.25 to 1.75
- router_weight: bfloat16 [1440, 16], replicated, may hold values from -0.15625 to 0.15625
- gate_weight: bfloat16 [1440, 23040], P(None, 'seq'), may hold values from -0.15625 to 0.15625
- up_weight: bfloat16 [1440, 23040], P(None, 'seq'), may hold values from -0.15625 to 0.15625
- down_weight: bfloat16 [23040, 1440], P('seq'), may hold values from -0.15625 to 0.15625
- routing: int32 [2, 1024, 2], P('fsdp', 'seq'), may hold values from 0 to 15, as said below
- span_order: int32 [32], replicated, may hold values from 0 to 31, as said below
Outputs:
- attended: bfloat16 [2, 1024, 1440], P('fsdp', 'seq')
- layer_output: bfloat16 [2, 1024, 1440], P('fsdp', 'seq')
The draws below stay inside these ranges and needn't reach their ends.
Inputs may be any that keep to these rules, and one draw needn't show every extreme that they name: A permutation of 0 to 31; index i of seq holds the rows of spans span_order[2 i] and span_order[2 i + 1], and these two add up to 31. `routing`: in the rows of one device no expert is named more than 12 times; in each prompt one expert is named exactly 12 times in the rows of every device; the 2 experts of a row differ.
All inputs are finite; a program needn't handle non-finite values.
Results may differ from the reference program's by a relative error of at most 0.009.
Values may be sent and summed in bfloat16 or wider, within the bound.
No kernel may reach another device: no remote copies, remote signals or barrier semaphores. Data moves between devices by JAX's collectives and lax.ppermute only.
A program may use at most 64 MiB of HBM per device.

```python
import jax
import jax.numpy as jnp
from jax import lax

D = 1440
HEADS = 32
KVH = 4
HD = 64
EXPERTS = 16
FFE = 1440
TOPK = 2
TOK_DEV = 64
HALF = 32
CAP = 12
PROMPTS = 2
TOKENS = 1024
SPANS = 32
UNITS = 1440
N_SEQ = 16


def draw_residual(key, part):
    noise_part = jax.random.normal(jax.random.fold_in(key, 7), (PROMPTS, TOKENS, D), jnp.float32)
    return jnp.clip(noise_part, -40.0, 40.0).astype(jnp.bfloat16)


def draw_queries(key, part):
    noise_key = jax.random.fold_in(key, 3)
    drawn = jax.random.normal(noise_key, (PROMPTS, TOKENS, HEADS, HD), jnp.float32)
    return jnp.clip(drawn, -64.0, 64.0).reshape(PROMPTS, TOKENS, HEADS * HD).astype(jnp.bfloat16)


def draw_key_rows(key, part):
    noise_key = jax.random.fold_in(key, 5)
    drawn = jax.random.normal(noise_key, (PROMPTS, TOKENS, KVH, HD), jnp.float32)
    return jnp.clip(drawn, -16.0, 16.0).reshape(PROMPTS, TOKENS, KVH * HD).astype(jnp.bfloat16)


def draw_span_order(key, part):
    pair_index = jax.random.permutation(jax.random.fold_in(key, 21), SPANS // 2).astype(jnp.int32)
    flip_order = jax.random.randint(jax.random.fold_in(key, 22), (SPANS // 2,), 0, 2).astype(jnp.int32)
    first_span = jnp.where(flip_order == 1, SPANS - 1 - pair_index, pair_index)
    return jnp.stack([first_span, SPANS - 1 - first_span], axis=1).reshape(SPANS).astype(jnp.int32)


def route_block(block_key, hot_expert):
    perm_key, order_key, turn_key = jax.random.split(block_key, 3)
    spare_slots = jax.random.permutation(perm_key, (EXPERTS - 1) * CAP)[:TOK_DEV * TOPK - CAP]
    others = (jnp.sort(spare_slots) // CAP).astype(jnp.int32)
    others = others + (others >= hot_expert).astype(jnp.int32)
    listed = jnp.concatenate([jnp.full((CAP,), hot_expert, jnp.int32), others])
    table_rows = listed.reshape(TOPK, TOK_DEV).T
    table_rows = table_rows[jax.random.permutation(order_key, TOK_DEV)]
    turn_by = jax.random.randint(turn_key, (TOK_DEV, 1), 0, TOPK)
    column_order = (jnp.arange(TOPK, dtype=jnp.int32)[None, :] + turn_by) % TOPK
    return jnp.take_along_axis(table_rows, column_order, axis=1).astype(jnp.int32)


def draw_routing(key, part):
    blocks = TOKENS // TOK_DEV
    hot_experts = jax.random.randint(jax.random.fold_in(key, 31), (PROMPTS,), 0, EXPERTS).astype(jnp.int32)
    block_keys = jax.random.split(jax.random.fold_in(key, 32), PROMPTS * blocks)
    hot_each = jnp.repeat(hot_experts, blocks)
    tables = jax.vmap(route_block)(block_keys, hot_each)
    return tables.reshape(PROMPTS, TOKENS, TOPK).astype(jnp.int32)


def steps_of(own_key, dims, pieces, low, top_value):
    def one(axis_at, shards_of):
        steps = jax.random.uniform(jax.random.fold_in(jax.random.fold_in(own_key, 6), axis_at), (shards_of,), jnp.float32, low / len(pieces), top_value / len(pieces))
        return jnp.repeat(jnp.exp(steps), dims[axis_at] // shards_of).reshape((-1,) + (1,) * (len(dims) - axis_at - 1))

    level = one(*pieces[0])
    for cut in pieces[1:]:
        level = level * one(*cut)
    return level


def gaussian(stream_key, dims, scale, bound, shards=(), kind=jnp.bfloat16):
    values = jax.random.normal(stream_key, dims, jnp.float32) * scale
    if len(shards) > 0:
        values = steps_of(stream_key, dims, shards, -0.22, 0.18) * values
    return jnp.clip(values, min=-bound, max=bound).astype(kind)


def setup_inputs(seed: int = 0) -> dict:
    splits = jax.random.split(jax.random.key(seed), 14)
    residual = draw_residual(jax.random.fold_in(splits[13], 71), 0)
    queries = draw_queries(jax.random.fold_in(splits[13], 71), 0)
    key_rows = draw_key_rows(jax.random.fold_in(splits[13], 71), 0)
    values = jnp.clip(-1.0 + 3.0 * jax.random.uniform(splits[3], (PROMPTS, TOKENS, KVH * HD), jnp.float32) ** steps_of(splits[3], (PROMPTS, TOKENS, KVH * HD), ((0, 2), (1, 16)), -0.2, 0.2), -1.0, 2.0).astype(jnp.bfloat16)
    attention_sinks = jnp.clip(jax.random.uniform(splits[4], (HEADS,), jnp.float32, 0.0, 6.0), 0.0, 6.0)
    out_weight = gaussian(splits[5], (HEADS * HD, D), (HEADS * HD) ** -0.5, 0.125, ((0, 16), (1, 2)))
    norm_gain = jnp.clip(1.0 + 0.15 * jax.random.normal(splits[6], (D,), jnp.float32), 0.25, 1.75).astype(jnp.bfloat16)
    router_weight = gaussian(splits[7], (D, EXPERTS), D ** -0.5, 0.15625)
    gate_weight = gaussian(splits[8], (D, EXPERTS * FFE), D ** -0.5, 0.15625, ((1, 16),))
    up_weight = gaussian(splits[9], (D, EXPERTS * FFE), D ** -0.5, 0.15625, ((1, 16),))
    down_weight = gaussian(splits[10], (EXPERTS * FFE, D), FFE ** -0.5, 0.15625, ((0, 16),))
    routing = draw_routing(jax.random.fold_in(splits[13], 71), 0)
    span_order = draw_span_order(jax.random.fold_in(splits[13], 71), 0)
    return dict(residual=residual, queries=queries, key_rows=key_rows, values=values, attention_sinks=attention_sinks, out_weight=out_weight, norm_gain=norm_gain, router_weight=router_weight, gate_weight=gate_weight, up_weight=up_weight, down_weight=down_weight, routing=routing, span_order=span_order)


rope_base = 150000.0
norm_eps = 1e-05
masked_score = -1e+30

def lookup(table_values, lookup_index):
    matches = lookup_index[:, None] == jnp.arange(table_values.shape[0], dtype=jnp.int32)[None, :]
    return lax.optimization_barrier(jnp.sum(jnp.where(matches, table_values[None, :], 0), axis=1)).astype(jnp.int32)

def positions(span_order, row_index):
    device = row_index // TOK_DEV
    within = row_index % TOK_DEV
    span_index = lookup(span_order, 2 * device + within // HALF)
    return span_index * HALF + within % HALF

def rotate(head_values, where_at):
    half_size = head_values.shape[-1] // 2
    frequency = jnp.exp(-jnp.log(rope_base) * jnp.arange(half_size, dtype=jnp.float32) / half_size)
    angles = where_at.astype(jnp.float32)[:, None] * frequency[None, :]
    cosine = jnp.cos(angles)[:, None, :]
    sine_part = jnp.sin(angles)[:, None, :]
    first_half = head_values[..., :half_size]
    second = head_values[..., half_size:]
    return jnp.concatenate([first_half * cosine - second * sine_part, second * cosine + first_half * sine_part], axis=-1)

def slot_of(chosen):
    flattened = chosen.reshape(-1)
    onehot = (flattened[:, None] == jnp.arange(EXPERTS, dtype=jnp.int32)[None, :]).astype(jnp.int32)
    before = jnp.cumsum(onehot, axis=0) - onehot
    return lax.optimization_barrier(jnp.sum(before * onehot, axis=1)).reshape(chosen.shape).astype(jnp.int32)

def reference(residual, queries, key_rows, values, attention_sinks, out_weight, norm_gain, router_weight, gate_weight, up_weight, down_weight, routing, span_order):
    where_at = positions(span_order, jnp.arange(TOKENS, dtype=jnp.int32))
    visible = where_at[None, :] <= where_at[:, None]
    score_scale = HD ** (-0.5)
    group_size = HEADS // KVH

    def attend_prompt(operands):
        query_prompt, key_prompt, value_prompt = operands
        query_rot = rotate(query_prompt.astype(jnp.float32).reshape(TOKENS, HEADS, HD), where_at).astype(jnp.bfloat16)
        key_rot = rotate(key_prompt.astype(jnp.float32).reshape(TOKENS, KVH, HD), where_at).astype(jnp.bfloat16)
        value_heads = value_prompt.reshape(TOKENS, KVH, HD)

        def attend_head(head_index):
            group_index = head_index // group_size
            query_one = lax.dynamic_index_in_dim(query_rot, head_index, 1, keepdims=False).astype(jnp.float32)
            key_one = lax.dynamic_index_in_dim(key_rot, group_index, 1, keepdims=False).astype(jnp.float32)
            value_one = lax.dynamic_index_in_dim(value_heads, group_index, 1, keepdims=False)
            sink_one = lax.dynamic_index_in_dim(attention_sinks, head_index, 0, keepdims=False).astype(jnp.float32)
            scores = jnp.dot(query_one, key_one.T, preferred_element_type=jnp.float32, precision=lax.Precision.HIGHEST) * score_scale
            scores = jnp.where(visible, scores, masked_score)
            row_max = jnp.maximum(lax.optimization_barrier(jnp.max(scores, axis=1)), sink_one)
            weight = jnp.exp(scores - row_max[:, None])
            denominator = lax.optimization_barrier(jnp.sum(weight, axis=1)) + jnp.exp(sink_one - row_max)
            weighted = jnp.dot(weight.astype(jnp.bfloat16), value_one, preferred_element_type=jnp.float32)
            return weighted / denominator[:, None]
        heads_out = lax.map(attend_head, jnp.arange(HEADS, dtype=jnp.int32))
        return jnp.transpose(heads_out, (1, 0, 2)).reshape(TOKENS, HEADS * HD).astype(jnp.bfloat16)
    attention_rows = lax.map(attend_prompt, (queries, key_rows, values))
    attended = jnp.dot(attention_rows.reshape(PROMPTS * TOKENS, HEADS * HD), out_weight, preferred_element_type=jnp.float32).astype(jnp.bfloat16)
    attended = attended.reshape(PROMPTS, TOKENS, D)
    stream = residual.astype(jnp.float32) + attended.astype(jnp.float32)
    normed = (stream * lax.rsqrt(lax.optimization_barrier(jnp.mean(stream * stream, axis=-1, keepdims=True)) + norm_eps) * norm_gain.astype(jnp.float32)).astype(jnp.bfloat16)
    logits = jnp.dot(normed.reshape(PROMPTS * TOKENS, D), router_weight, preferred_element_type=jnp.float32).reshape(PROMPTS, TOKENS, EXPERTS)
    selected = jnp.take_along_axis(logits, routing, axis=-1)
    gates = 1.0 / lax.optimization_barrier(jnp.sum(jnp.exp(selected[..., :, None] - selected[..., None, :]), axis=-2))

    def expert_prompt(operands):
        normed_prompt, chosen_prompt, gates_prompt = operands
        blocks_in = normed_prompt.reshape(N_SEQ, TOK_DEV, D)
        chosen_blocks = chosen_prompt.reshape(N_SEQ, TOK_DEV, TOPK)
        slot_blocks = jax.vmap(slot_of)(chosen_blocks)
        target = chosen_blocks * CAP + slot_blocks

        def dispatch_one(target_block, rows_block):
            mapping = lax.optimization_barrier(jnp.sum((target_block[None, :, :] == jnp.arange(EXPERTS * CAP, dtype=jnp.int32)[:, None, None]).astype(jnp.int32), axis=2))
            return jnp.dot(mapping.astype(jnp.bfloat16), rows_block, preferred_element_type=jnp.float32).astype(jnp.bfloat16)
        buffers = jax.vmap(dispatch_one)(target, blocks_in).reshape(N_SEQ, EXPERTS, CAP, D)

        def run_one(expert_index):
            expert_rows = lax.dynamic_index_in_dim(buffers, expert_index, 1, keepdims=False).reshape(N_SEQ * CAP, D)
            gate_columns = lax.dynamic_slice_in_dim(gate_weight, (expert_index * FFE).astype(jnp.int32), FFE, 1)
            up_columns = lax.dynamic_slice_in_dim(up_weight, (expert_index * FFE).astype(jnp.int32), FFE, 1)
            down_rows = lax.dynamic_slice_in_dim(down_weight, (expert_index * FFE).astype(jnp.int32), FFE, 0)
            gate_values = jnp.dot(expert_rows, gate_columns, preferred_element_type=jnp.float32)
            up_values = jnp.dot(expert_rows, up_columns, preferred_element_type=jnp.float32)
            hidden = (gate_values * jax.nn.sigmoid(1.702 * gate_values) * (up_values + 1.0)).astype(jnp.bfloat16)
            parts = jnp.einsum('rgu,gud->rgd', hidden.reshape(N_SEQ * CAP, FFE // UNITS, UNITS).astype(jnp.float32), down_rows.reshape(FFE // UNITS, UNITS, D).astype(jnp.float32))
            rounded = lax.optimization_barrier(parts.astype(jnp.bfloat16))
            return lax.optimization_barrier(jnp.sum(rounded.astype(jnp.float32), axis=1))
        outputs = lax.map(run_one, jnp.arange(EXPERTS, dtype=jnp.int32)).reshape(EXPERTS * N_SEQ * CAP, D)
        device_index = jnp.arange(N_SEQ, dtype=jnp.int32)[:, None, None]
        flat_index = ((chosen_blocks * N_SEQ + device_index) * CAP + slot_blocks).reshape(-1).astype(jnp.int32)
        chosen_out = jnp.take(outputs, flat_index, axis=0).reshape(TOKENS, TOPK, D)
        return lax.optimization_barrier(jnp.sum(chosen_out * gates_prompt[:, :, None], axis=1))
    expert_mix = lax.map(expert_prompt, (normed, routing, gates))
    layer_output = (stream + expert_mix).astype(jnp.bfloat16)
    return (attended, layer_output)
```

```python
import functools
import jax
import jax.numpy as jnp
from jax import lax
from jax.experimental import pallas as pl
from jax.experimental.pallas import tpu as pltpu
from jax.sharding import PartitionSpec as P

KVH = 4
HD = 64
EXPERTS = 16
TOPK = 2
HALF = 32
CAP = 12


rope_base = 150000.0
norm_eps = 1e-05
masked_score = -1e30
PLANE = 4

vmem = pl.BlockSpec(memory_space=pltpu.VMEM)
smem = pl.BlockSpec(memory_space=pltpu.SMEM)
anym = pl.BlockSpec(memory_space=pl.ANY)
params = pltpu.CompilerParams(vmem_limit_bytes=56 * 1024 * 1024)


def shift(value, axis, source_to):
    count = lax.axis_size(axis)
    return lax.ppermute(value, axis, [(i, source_to(i)) for i in range(count)])


def gather_pieces(own):
    count = lax.axis_size("seq")
    lines = count // PLANE
    pieces = [own]
    for d in range(1, lines):
        pieces.append(shift(own, "seq", lambda i, d=d: (i + PLANE * d) % count))
    pieces = pieces + [shift(piece, "seq", lambda i: i ^ 2) for piece in pieces]
    return pieces + [shift(piece, "seq", lambda i: i ^ 1) for piece in pieces]


def piece_owners():
    count = lax.axis_size("seq")
    lines = count // PLANE
    me = lax.axis_index("seq")
    order = jnp.arange(count, dtype=jnp.int32)
    back = order % lines
    flip_y = (order // lines) % 2
    flip_core = order // (2 * lines)
    line = (me // PLANE - back + lines) % lines
    plane = (me % PLANE) ^ (flip_y * 2 + flip_core)
    return line * PLANE + plane


def rope(first, second, cosine, sine):
    return jnp.concatenate(
        [first * cosine - second * sine, second * cosine + first * sine], axis=-1
    )


def prepare_kernel(spans, keys, values, frequency, out, cosine_out, sine_out):
    rows = keys.shape[0]
    row = lax.broadcasted_iota(jnp.int32, (rows, HD // 2), 0)
    where_at = jnp.where(
        row < HALF, spans[0] * HALF + row, spans[1] * HALF + row - HALF
    ).astype(jnp.float32)
    angles = where_at * frequency[...]
    cosine = jnp.cos(angles)
    sine = jnp.sin(angles)
    cosine_out[...] = cosine
    sine_out[...] = sine
    width = keys.shape[1]
    for head in range(width // HD):
        one = keys[:, head * HD : (head + 1) * HD].astype(jnp.float32)
        rotated = rope(one[:, : HD // 2], one[:, HD // 2 :], cosine, sine)
        out[:, head * HD : (head + 1) * HD] = rotated.astype(jnp.bfloat16)
    out[:, width:] = values[...]


def attention_kernel(*refs, piece_count):
    sinks, queries, cosine, sine, query_at, key_at = refs[:6]
    pieces = refs[6 : 6 + piece_count]
    out, gathered = refs[6 + piece_count :]
    rows = queries.shape[0]
    piece_rows = pieces[0].shape[0]
    group = queries.shape[1] // (KVH * HD)
    for index, piece in enumerate(pieces):
        gathered[index * piece_rows : (index + 1) * piece_rows, :] = piece[...]
    bias = jnp.where(key_at[...] <= query_at[...], 0.0, masked_score)
    cos = cosine[...]
    sin = sine[...]
    for kv in range(KVH):
        key = gathered[:, kv * HD : (kv + 1) * HD]
        value = gathered[:, (KVH + kv) * HD : (KVH + kv + 1) * HD]
        stacked = []
        sink_rows = []
        for j in range(group):
            head = kv * group + j
            one = queries[:, head * HD : (head + 1) * HD].astype(jnp.float32)
            rotated = rope(one[:, : HD // 2], one[:, HD // 2 :], cos, sin).astype(jnp.bfloat16)
            stacked.append(rotated)
            sink_rows.append(jnp.full((rows, 1), sinks[head], jnp.float32))
        query = jnp.concatenate(stacked, axis=0) * jnp.bfloat16(HD ** (-0.5))
        sink = jnp.concatenate(sink_rows, axis=0)
        scores = lax.dot_general(
            query, key, (((1,), (1,)), ((), ())), preferred_element_type=jnp.float32
        )
        scores = (scores.reshape(group, rows, -1) + bias[None]).reshape(group * rows, -1)
        top = jnp.maximum(jnp.max(scores, axis=1, keepdims=True), sink)
        weights = jnp.exp(scores - top)
        total = jnp.sum(weights, axis=1, keepdims=True) + jnp.exp(sink - top)
        mixed = jnp.dot(weights.astype(jnp.bfloat16), value, preferred_element_type=jnp.float32)
        mixed = (mixed / total).astype(jnp.bfloat16)
        for j in range(group):
            head = kv * group + j
            out[:, head * HD : (head + 1) * HD] = mixed[j * rows : (j + 1) * rows]


def project_kernel(*refs):
    owners, rows = refs[:2]
    pieces = refs[2:-1]
    out = refs[-1]
    width = pieces[0].shape[0]
    total = jnp.zeros(out.shape, jnp.float32)
    for index, piece in enumerate(pieces):
        start = pl.multiple_of(owners[index] * width, width)
        total = total + jnp.dot(
            rows[:, pl.ds(start, width)], piece[...], preferred_element_type=jnp.float32
        )
    out[...] = total.astype(jnp.bfloat16)


def expert_kernel(arrived, pick, place, gate_hbm, up_hbm, down_hbm, out, gate, up, down, sems):
    half = arrived.shape[1]
    copies = []
    for index, (source, target) in enumerate(((gate_hbm, gate), (up_hbm, up))):
        for part in range(2):
            window = pl.ds(part * half, half)
            copies.append(
                pltpu.make_async_copy(
                    source.at[window], target.at[window], sems.at[2 * index + part]
                )
            )
    copies.append(pltpu.make_async_copy(down_hbm, down, sems.at[4]))
    for copy in copies:
        copy.start()
    picked = jnp.dot(pick[...], arrived[...], preferred_element_type=jnp.float32).astype(
        jnp.bfloat16
    )
    slots = picked.shape[0] // 2
    first = picked[:slots]
    second = picked[slots:]
    copies[0].wait()
    gate_values = jnp.dot(first, gate[:half], preferred_element_type=jnp.float32)
    copies[1].wait()
    gate_values += jnp.dot(second, gate[half:], preferred_element_type=jnp.float32)
    copies[2].wait()
    up_values = jnp.dot(first, up[:half], preferred_element_type=jnp.float32)
    copies[3].wait()
    up_values += jnp.dot(second, up[half:], preferred_element_type=jnp.float32)
    hidden = (gate_values * jax.nn.sigmoid(1.702 * gate_values) * (up_values + 1.0)).astype(
        jnp.bfloat16
    )
    copies[4].wait()
    result = jnp.dot(hidden, down[...], preferred_element_type=jnp.float32).astype(jnp.bfloat16)
    both = jnp.concatenate([result[:, :half], result[:, half:]], axis=0)
    out[...] = jnp.dot(place[...], both, preferred_element_type=jnp.float32).astype(jnp.bfloat16)


def mix_kernel(stream, gates, choose, returned, out):
    rows = stream.shape[0]
    half = returned.shape[1]
    taken = jnp.dot(choose[...], returned[...], preferred_element_type=jnp.float32)
    for part in range(2):
        mixed = stream[:, part * half : (part + 1) * half]
        for j in range(TOPK):
            at = (part * TOPK + j) * rows
            mixed = mixed + taken[at : at + rows] * gates[:, j : j + 1]
        out[:, part * half : (part + 1) * half] = mixed.astype(jnp.bfloat16)


def slot_of(chosen):
    flattened = chosen.reshape(-1)
    onehot = (flattened[:, None] == jnp.arange(EXPERTS, dtype=jnp.int32)[None, :]).astype(
        jnp.float32
    )
    count = flattened.shape[0]
    earlier = (
        jnp.arange(count, dtype=jnp.int32)[None, :] < jnp.arange(count, dtype=jnp.int32)[:, None]
    )
    before = jnp.dot(
        earlier.astype(jnp.bfloat16), onehot.astype(jnp.bfloat16), preferred_element_type=jnp.float32
    )
    return jnp.sum(before * onehot, axis=1).astype(jnp.int32).reshape(chosen.shape)


def on_device(
    residual,
    queries,
    key_rows,
    values,
    attention_sinks,
    out_weight,
    norm_gain,
    router_weight,
    gate_weight,
    up_weight,
    down_weight,
    routing,
    span_order,
):
    seq_count = lax.axis_size("seq")
    fsdp_count = lax.axis_size("fsdp")
    seq_index = lax.axis_index("seq")
    fsdp_index = lax.axis_index("fsdp")
    token_count = residual.shape[1]
    width = residual.shape[2]
    half = width // 2
    bf16 = jnp.bfloat16

    spans = lax.dynamic_slice_in_dim(span_order, 2 * seq_index, 2)
    frequency = jnp.exp(
        -jnp.log(rope_base) * jnp.arange(HD // 2, dtype=jnp.float32) / (HD // 2)
    )[None, :]
    angle_shape = jax.ShapeDtypeStruct((token_count, HD // 2), jnp.float32)
    kv_width = key_rows.shape[2]
    kv_own, cosine, sine = pl.pallas_call(
        prepare_kernel,
        out_shape=(
            jax.ShapeDtypeStruct((token_count, 2 * kv_width), bf16),
            angle_shape,
            angle_shape,
        ),
        in_specs=[smem, vmem, vmem, vmem],
        out_specs=(vmem, vmem, vmem),
        compiler_params=params,
        name="prepare",
    )(spans, key_rows[0], values[0], frequency)

    kv_pieces = gather_pieces(kv_own)
    owners = piece_owners()
    within = jnp.arange(token_count, dtype=jnp.int32)
    span_pairs = span_order.reshape(seq_count, 2)
    owned = owners[:, None] == jnp.arange(seq_count, dtype=jnp.int32)[None, :]
    piece_spans = jnp.sum(jnp.where(owned[:, :, None], span_pairs[None], 0), axis=1)
    key_at = jnp.where(
        within[None, :] < HALF,
        piece_spans[:, :1] * HALF + within[None, :],
        piece_spans[:, 1:] * HALF + within[None, :] - HALF,
    ).reshape(1, seq_count * token_count)
    query_at = jnp.where(
        within < HALF, spans[0] * HALF + within, spans[1] * HALF + within - HALF
    )[:, None]
    attention_rows = pl.pallas_call(
        functools.partial(attention_kernel, piece_count=seq_count),
        out_shape=jax.ShapeDtypeStruct(queries.shape[1:], bf16),
        in_specs=[smem] + [vmem] * (5 + seq_count),
        out_specs=vmem,
        scratch_shapes=[pltpu.VMEM((seq_count * token_count, 2 * kv_width), bf16)],
        compiler_params=params,
        name="attend",
    )(attention_sinks, queries[0], cosine, sine, query_at, key_at, *kv_pieces)

    weight_pieces = gather_pieces(out_weight)
    feature_rows, columns = out_weight.shape

    if feature_rows % 128 == 0:

        def project(rows):
            return pl.pallas_call(
                project_kernel,
                out_shape=jax.ShapeDtypeStruct((token_count, columns), bf16),
                in_specs=[smem, vmem] + [vmem] * seq_count,
                out_specs=vmem,
                compiler_params=params,
                name="project",
            )(owners, rows, *weight_pieces)
    else:
        ordered = jnp.concatenate(weight_pieces, axis=0).reshape(seq_count, feature_rows, columns)
        inverse = jnp.argmax(owned, axis=0)
        ordered = jnp.take(ordered, inverse, axis=0).reshape(seq_count * feature_rows, columns)

        def project(rows):
            return jnp.dot(rows, ordered, preferred_element_type=jnp.float32).astype(bf16)

    blocks = []
    others = [
        shift(attention_rows, "fsdp", lambda i, d=d: (i + d) % fsdp_count)
        for d in range(1, fsdp_count)
    ]
    blocks.append(project(attention_rows))
    for d in range(1, fsdp_count):
        blocks.append(
            shift(project(others[d - 1]), "fsdp", lambda i, d=d: (i - d) % fsdp_count)
        )
    ordered_blocks = []
    for block in range(fsdp_count):
        picked = blocks[0]
        for d in range(1, fsdp_count):
            picked = jnp.where((fsdp_index + d) % fsdp_count == block, blocks[d], picked)
        ordered_blocks.append(picked)
    attended = jnp.concatenate(ordered_blocks, axis=1)

    stream = residual[0].astype(jnp.float32) + attended.astype(jnp.float32)
    normed = (
        stream
        * lax.rsqrt(jnp.mean(stream * stream, axis=-1, keepdims=True) + norm_eps)
        * norm_gain.astype(jnp.float32)
    ).astype(bf16)
    logits = jnp.dot(normed, router_weight, preferred_element_type=jnp.float32)
    chosen = routing[0]
    matches = chosen[:, :, None] == jnp.arange(EXPERTS, dtype=jnp.int32)[None, None, :]
    chosen_logits = jnp.sum(jnp.where(matches, logits[:, None, :], 0.0), axis=-1)
    gates = 1.0 / jnp.sum(jnp.exp(chosen_logits[:, :, None] - chosen_logits[:, None, :]), axis=1)
    slot_index = slot_of(chosen)

    def row_of(expert, slot, part):
        return expert * (2 * CAP) + part * CAP + slot

    out_rows = EXPERTS * 2 * CAP
    row_ids = jnp.arange(out_rows, dtype=jnp.int32)
    first_row = row_of(chosen, slot_index, 0)
    target = jnp.concatenate([first_row, first_row + CAP], axis=0)
    dispatch_map = (target[None, :, 0] == row_ids[:, None]) | (
        target[None, :, 1] == row_ids[:, None]
    )
    halves = jnp.concatenate([normed[:, :half], normed[:, half:]], axis=0)
    buffer = jnp.dot(dispatch_map.astype(bf16), halves, preferred_element_type=jnp.float32).astype(
        bf16
    )
    copies = seq_count // EXPERTS
    outgoing = jnp.broadcast_to(
        buffer.reshape(EXPERTS, 1, 2 * CAP, half), (EXPERTS, copies, 2 * CAP, half)
    ).reshape(seq_count, 2 * CAP, half)
    arrived = lax.all_to_all(outgoing, "seq", split_axis=0, concat_axis=0, tiled=True)

    total_rows = seq_count * 2 * CAP
    slots = jnp.arange(seq_count * CAP, dtype=jnp.int32)
    slot_rows = slots // CAP * (2 * CAP) + slots % CAP
    pick_rows = jnp.concatenate([slot_rows, slot_rows + CAP])
    arrived_ids = jnp.arange(total_rows, dtype=jnp.int32)
    pick = (pick_rows[:, None] == arrived_ids[None, :]).astype(bf16)
    place = (pick_rows[None, :] == arrived_ids[:, None]).astype(bf16)
    returned = pl.pallas_call(
        expert_kernel,
        out_shape=jax.ShapeDtypeStruct((total_rows, half), bf16),
        in_specs=[vmem, vmem, vmem, anym, anym, anym],
        out_specs=vmem,
        scratch_shapes=[
            pltpu.VMEM(gate_weight.shape, bf16),
            pltpu.VMEM(up_weight.shape, bf16),
            pltpu.VMEM(down_weight.shape, bf16),
            pltpu.SemaphoreType.DMA((5,)),
        ],
        compiler_params=params,
        name="experts",
    )(arrived.reshape(total_rows, half), pick, place, gate_weight, up_weight, down_weight)
    returned = lax.all_to_all(
        returned.reshape(seq_count, 2 * CAP, half),
        "seq",
        split_axis=0,
        concat_axis=0,
        tiled=True,
    ).reshape(total_rows, half)

    block_rows = copies * 2 * CAP
    source_row = arrived_ids // block_rows * (2 * CAP) + arrived_ids % (2 * CAP)
    wanted = jnp.concatenate(
        [first_row[:, j] + part * CAP for part in range(2) for j in range(TOPK)]
    )
    choose = (wanted[:, None] == source_row[None, :]).astype(bf16)
    layer_output = pl.pallas_call(
        mix_kernel,
        out_shape=jax.ShapeDtypeStruct((token_count, width), bf16),
        in_specs=[vmem] * 4,
        out_specs=vmem,
        compiler_params=params,
        name="mix",
    )(stream, gates, choose, returned)
    return (attended[None], layer_output[None])


def solution(mesh):
    in_specs = (
        P("fsdp", "seq", None),
        P("fsdp", "seq", None),
        P("fsdp", "seq", None),
        P("fsdp", "seq", None),
        P(),
        P("seq", "fsdp"),
        P(),
        P(),
        P(None, "seq"),
        P(None, "seq"),
        P("seq", None),
        P("fsdp", "seq", None),
        P(),
    )
    out_specs = (P("fsdp", "seq", None), P("fsdp", "seq", None))
    return jax.shard_map(
        on_device, mesh=mesh, in_specs=in_specs, out_specs=out_specs, check_vma=False
    )
```
